32 devices in a mesh: col: 16 (over z, y, x), lev: 2 (over core).
Axes of the slice: x: 2, y: 2, z: 4, core: 2. Of those that a mesh axis runs over, the one named last changes fastest.
Arguments:
- perturbations: float32 [80, 16, 16384], P(None, 'lev', 'col'), may hold values from -0.625 to 0.625
- gradient: float32 [32, 16, 16384], P(None, 'lev', 'col'), may hold values from -2 to 2
- horizontal: float32 [20, 16384], P(None, 'col'), may hold values from -50 to 50
- area: float32 [16384], P('col'), may hold values from 1 to 60
- vertical: float32 [20, 16], P(None, 'lev'), may hold values from -1.25 to 1.25
Outputs:
- increment: float32 [32, 16, 16384], P(None, 'lev', 'col')
- background: float32 [32], replicated
The draws below stay inside these ranges and needn't reach their ends.
All inputs are finite; a program needn't handle non-finite values.
Results may differ from the reference program's by a relative error of at most 0.0003.
Values sent between devices are 32-bit elements; how exact they have to be, the bound alone decides.
A program may use at most 128 MiB of HBM per device.

```python
import math
import jax
import jax.numpy as jnp
from jax import lax

MEMBERS = 80
VMODES = 20
HMODES = 20
VECTORS = 32
LEV = 16
COLS = 16384


def draw_area(key, part):
    position = jnp.arange(COLS).astype(jnp.float32)
    ramped = 1.0 + 2.0 * position / max(COLS - 1, 1)
    rough = jnp.exp(jax.random.uniform(key, (COLS,), jnp.float32, 0.0, math.log(10.0)))
    return ramped * rough


def draw_horizontal(key, part):
    first, second = jax.random.split(jax.random.fold_in(key, 17), 2)
    row_scale = jnp.exp(jax.random.uniform(first, (HMODES, 1), jnp.float32, 0.0, math.log(10.0)))
    column_values = jnp.clip(jax.random.normal(second, (HMODES, COLS), jnp.float32), -5.0, 5.0)
    return row_scale * column_values


def shard_levels(key, dims, cuts, least, top_value):
    def one(dim, blocks):
        draws = jax.random.uniform(jax.random.fold_in(jax.random.fold_in(key, 6), dim), (blocks,), jnp.float32, least / len(cuts), top_value / len(cuts))
        return jnp.repeat(jnp.exp(draws), dims[dim] // blocks).reshape((-1,) + (1,) * (len(dims) - dim - 1))

    factor_of = one(*cuts[0])
    for cut in cuts[1:]:
        factor_of = factor_of * one(*cut)
    return factor_of


def centred(key, extent, width, bound, shards=(), dtype=jnp.bfloat16):
    values = width * jax.random.normal(key, extent, jnp.float32)
    if shards:
        values = values * shard_levels(key, extent, shards, -0.22, 0.18)
    return jnp.clip(values, -bound, bound).astype(dtype)


def setup_inputs(seed: int = 0) -> dict:
    seeds = jax.random.split(jax.random.key(seed), 6)
    return {
        "perturbations": centred(seeds[0], (MEMBERS, LEV, COLS), MEMBERS ** -0.5, 0.625, ((1, 2), (2, 16)), jnp.float32),
        "gradient": centred(seeds[1], (VECTORS, LEV, COLS), (max(1, LEV * COLS // (VMODES * HMODES * MEMBERS))) ** -0.5, 2.0, ((1, 2), (2, 16)), jnp.float32),
        "horizontal": draw_horizontal(jax.random.fold_in(seeds[5], 71), 0),
        "area": draw_area(jax.random.fold_in(seeds[5], 71), 0),
        "vertical": centred(seeds[4], (VMODES, LEV), VMODES ** -0.5, 1.25, ((1, 2),), jnp.float32),
    }


TOP_PRECISION = lax.Precision.HIGHEST

def reference(perturbations, gradient, horizontal, area, vertical):
    area_sum = jnp.sum(area)
    mode_power = lax.optimization_barrier(jnp.sum(area[None, :] * horizontal * horizontal, axis=1))
    scaled_terms = horizontal / jnp.sqrt(HMODES * (mode_power / area_sum + 1e-06))[:, None]
    weight = area * (COLS / area_sum)

    def adjoint_level(level_index):
        level_index = level_index.astype(jnp.int32)
        ensemble_member_rows = lax.dynamic_index_in_dim(perturbations, level_index, 1, keepdims=False)
        gradient_rows = lax.dynamic_index_in_dim(gradient, level_index, 1, keepdims=False)
        mode_products = (gradient_rows * weight[None, :])[:, None, :] * scaled_terms[None, :, :]
        return jnp.einsum('kc,vbc->kvb', ensemble_member_rows, mode_products, precision=TOP_PRECISION)
    terms = lax.map(adjoint_level, jnp.arange(LEV).astype(jnp.int32))
    control = jnp.einsum('al,lkvb->vkab', vertical, terms, precision=TOP_PRECISION)
    lifted = jnp.einsum('al,vkab->lkvb', vertical, control, precision=TOP_PRECISION)

    def forward_level_map(level_index):
        level_index = level_index.astype(jnp.int32)
        ensemble_member_rows = lax.dynamic_index_in_dim(perturbations, level_index, 1, keepdims=False)
        level_lift = lax.dynamic_index_in_dim(lifted, level_index, 0, keepdims=False)
        member_spread = jnp.einsum('kvb,kc->vbc', level_lift, ensemble_member_rows, precision=TOP_PRECISION)
        return lax.optimization_barrier(jnp.sum(member_spread * scaled_terms[None, :, :], axis=1))
    by_level = lax.map(forward_level_map, jnp.arange(LEV).astype(jnp.int32))
    increment = jnp.transpose(by_level, (1, 0, 2))
    background = 0.5 * lax.optimization_barrier(jnp.sum(control * control, axis=(1, 2, 3)))
    return (increment, background)
```

```python
import functools

import jax
import jax.numpy as jnp
from jax import lax
from jax.experimental import pallas as pl
from jax.experimental.pallas import tpu as pltpu
from jax.sharding import PartitionSpec as P

LANES = 128
NT = (((1,), (1,)), ((), ()))
TN = (((0,), (0,)), ((), ()))
NN = (((1,), (0,)), ((), ()))


def split(x):
    high = x.astype(jnp.bfloat16)
    low = (x - high.astype(jnp.float32)).astype(jnp.bfloat16)
    return high, low


def adjoint_kernel(sizes, pert_ref, grad_ref, hor_ref, area_ref, terms_ref, stat_ref):
    members, levels, vectors, modes, columns = sizes
    group = LANES // vectors
    chunks = modes // group
    used = chunks * members * levels
    if used < terms_ref.shape[0]:
        terms_ref[used:, :] = jnp.zeros((terms_ref.shape[0] - used, LANES), jnp.float32)
    area = area_ref[...]
    power = jnp.sum(area * hor_ref[...] * hor_ref[...], axis=1, keepdims=True)
    spread_power = jnp.broadcast_to(power, (modes, LANES))
    lane = lax.broadcasted_iota(jnp.int32, (modes, LANES), 1)
    row = lax.broadcasted_iota(jnp.int32, (modes, LANES), 0)
    powers = jnp.sum(jnp.where(lane == row, spread_power, 0.0), axis=0, keepdims=True)
    total = jnp.broadcast_to(jnp.sum(area, axis=1, keepdims=True), (1, LANES))
    stat_row = jnp.where(lane[:1] == modes, total, powers)
    stat_ref[...] = jnp.broadcast_to(stat_row, stat_ref.shape)

    def level(l, carry):
        high, low = split(pert_ref[:, l, :])
        both = jnp.concatenate([high, low], axis=0)
        weighted = grad_ref[:, l, :] * area
        for j in range(chunks):
            products = jnp.concatenate(
                [weighted * hor_ref[b : b + 1, :] for b in range(j * group, (j + 1) * group)],
                axis=0,
            )
            x = jnp.concatenate(split(products), axis=0)
            out = lax.dot_general(both, x, NT, preferred_element_type=jnp.float32)
            terms = out[:members, :LANES] + (out[members:, :LANES] + out[:members, LANES:])
            terms_ref[pl.ds(j * members * levels + l, members, stride=levels), :] = terms
        return carry

    for l in range(levels):
        level(l, 0)


def factor_column(stat, modes):
    lane = lax.broadcasted_iota(jnp.int32, (modes, LANES), 1)
    row = lax.broadcasted_iota(jnp.int32, (modes, LANES), 0)
    wide = jnp.broadcast_to(stat, (modes, LANES))
    power = jnp.sum(jnp.where(lane == row, wide, 0.0), axis=1, keepdims=True)
    area = jnp.sum(jnp.where(lane == modes, wide, 0.0), axis=1, keepdims=True)
    return 1.0 / jnp.sqrt(modes * (power / area + 1e-06)), area


def exchange_kernel(
    sizes, n, terms_ref, stat_ref, vert_ref, vert_t_ref, lifted_ref, parts_ref, total_ref,
    arrived, stats, reduced, verticals, weights,
    send_t, recv_t, send_s, recv_s, send_l, recv_l, send_b, recv_b, send_p, recv_p,
):
    members, levels, vectors, modes, columns = sizes
    group = LANES // vectors
    chunks = modes // group
    vmodes = vert_ref.shape[0]
    rows = terms_ref.shape[1]
    tiles = rows // levels
    me = lax.axis_index("col")
    lev = lax.axis_index("lev")
    other = 1 - lev
    mesh_id = pl.DeviceIdType.MESH
    barrier = pltpu.get_barrier_semaphore()

    def greet(p, carry):
        pl.semaphore_signal(
            barrier, inc=1, device_id=(lax.rem(me + p, n), lev), device_id_type=mesh_id
        )
        return carry

    lax.fori_loop(1, n, greet, 0)
    pl.semaphore_signal(barrier, inc=1, device_id=(me, other), device_id_type=mesh_id)
    pl.semaphore_wait(barrier, n)

    def remote(src, dst, send, recv, device):
        return pltpu.make_async_remote_copy(
            src_ref=src, dst_ref=dst, send_sem=send, recv_sem=recv,
            device_id=device, device_id_type=mesh_id,
        )

    def terms_copy(p):
        peer = lax.rem(me + p, n)
        return remote(terms_ref.at[peer], arrived.at[p], send_t.at[p], recv_t.at[p], (peer, lev))

    def stat_copy(p, slot):
        peer = lax.rem(me + p, n)
        return remote(stat_ref, stats.at[slot], send_s.at[p], recv_s.at[p], (peer, lev))

    def lifted_copy(p, slot):
        peer = lax.rem(me + p, n)
        return remote(
            lifted_ref.at[slot], lifted_ref.at[slot], send_l.at[p], recv_l.at[p], (peer, lev)
        )

    def part_copy(p, slot):
        peer = lax.rem(me + p, n)
        return remote(
            parts_ref.at[slot], parts_ref.at[slot], send_b.at[p], recv_b.at[p], (peer, lev)
        )

    def start_first(p, carry):
        stat_copy(p, me).start()
        terms_copy(p).start()
        return carry

    lax.fori_loop(1, n, start_first, 0)
    vert_copy = remote(
        vert_ref, verticals.at[lev], send_p.at[0], recv_p.at[0], (me, other)
    )
    vert_copy.start()
    stats[me] = stat_ref[...]
    verticals[lev] = vert_ref[...]
    reduced[lev] = terms_ref[me]

    def take(p, carry):
        stat_copy(p, lax.rem(me + n - p, n)).wait_recv()
        terms_copy(p).wait_recv()
        reduced[lev] += arrived[p]
        return carry

    lax.fori_loop(1, n, take, 0)
    pair_copy = remote(
        reduced.at[lev], reduced.at[lev], send_p.at[1], recv_p.at[1], (me, other)
    )
    pair_copy.start()

    def add_stat(i, carry):
        return carry + stats[i]

    stat = lax.fori_loop(0, n, add_stat, jnp.zeros(stat_ref.shape, jnp.float32))
    total_ref[...] = stat
    factor, area = factor_column(stat[:1], modes)
    factor = factor / area
    lane = lax.broadcasted_iota(jnp.int32, (modes, LANES), 1)
    row = lax.broadcasted_iota(jnp.int32, (modes, LANES), 0)
    placed = jnp.where(
        lax.div(lane, vectors) == lax.rem(row, group), jnp.broadcast_to(factor, lane.shape), 0.0
    )
    for j in range(chunks):
        weights[j : j + 1, :] = jnp.sum(
            placed[j * group : (j + 1) * group], axis=0, keepdims=True
        )
    remote(
        vert_ref, verticals.at[other], send_p.at[0], recv_p.at[0], (me, other)
    ).wait_recv()
    remote(
        reduced.at[lev], reduced.at[other], send_p.at[1], recv_p.at[1], (me, other)
    ).wait_recv()

    def wide(index):
        block = reduced[index]
        return jnp.concatenate(
            [block[i * levels : (i + 1) * levels] for i in range(tiles)], axis=1
        )

    def dot(a, b):
        return lax.dot_general(
            a, b, NN, precision=lax.Precision.HIGHEST, preferred_element_type=jnp.float32
        )

    control = dot(verticals[0][:, :levels], wide(0)) + dot(verticals[1][:, :levels], wide(1))
    lifted = dot(vert_t_ref[...][:, :vmodes], control)
    part = jnp.zeros((1, LANES), jnp.float32)
    for i in range(tiles):
        lifted_ref[me, i * levels : (i + 1) * levels, :] = lifted[:, i * LANES : (i + 1) * LANES]
        chunk = jnp.minimum(lax.div(me * tiles + i, members), chunks - 1)
        scaled = control[:, i * LANES : (i + 1) * LANES] * weights[pl.ds(chunk, 1), :]
        part = part + jnp.sum(scaled * scaled, axis=0, keepdims=True)
    parts_ref[me] = jnp.broadcast_to(part, parts_ref.shape[1:])

    def start_second(p, carry):
        lifted_copy(p, me).start()
        part_copy(p, me).start()
        return carry

    lax.fori_loop(1, n, start_second, 0)
    vert_copy.wait_send()
    pair_copy.wait_send()

    def finish(p, carry):
        source = lax.rem(me + n - p, n)
        stat_copy(p, me).wait_send()
        terms_copy(p).wait_send()
        lifted_copy(p, source).wait_recv()
        part_copy(p, source).wait_recv()
        lifted_copy(p, me).wait_send()
        part_copy(p, me).wait_send()
        return carry

    lax.fori_loop(1, n, finish, 0)


def forward_kernel(
    sizes, n, lifted_ref, parts_ref, total_ref, pert_ref, hor_ref, out_ref, bg_ref, scaled_ref
):
    members, levels, vectors, modes, columns = sizes
    group = LANES // vectors
    chunks = modes // group
    width = 256
    part = lax.fori_loop(
        0, n, lambda i, c: c + parts_ref[i], jnp.zeros(parts_ref.shape[1:], jnp.float32)
    )
    folded = part
    for g in range(1, group):
        folded = folded + pltpu.roll(part, g * vectors, 1)
    bg_ref[...] = 0.5 * folded
    factor, area = factor_column(total_ref[:1, :], modes)
    scaled_ref[...] = hor_ref[...] * (factor * (factor / area))

    def level(l, carry):
        lhs = []
        for j in range(chunks):
            high, low = split(
                lifted_ref[pl.ds(j * members * levels + l, members, stride=levels), :]
            )
            lhs.append(jnp.concatenate([high, low, high], axis=0))
        for c in range(0, columns, width):
            high, low = split(pert_ref[:, l, c : c + width])
            rhs = jnp.concatenate([high, high, low], axis=0)
            acc = None
            for j in range(chunks):
                spread = lax.dot_general(lhs[j], rhs, TN, preferred_element_type=jnp.float32)
                for g in range(group):
                    b = j * group + g
                    term = (
                        spread[g * vectors : (g + 1) * vectors]
                        * scaled_ref[b : b + 1, c : c + width]
                    )
                    acc = term if acc is None else acc + term
            out_ref[:, l, c : c + width] = acc
        return carry

    for l in range(levels):
        level(l, 0)


def per_device(perturbations, gradient, horizontal, area, vertical):
    members, levels, columns = perturbations.shape
    vectors = gradient.shape[0]
    modes = horizontal.shape[0]
    vmodes = vertical.shape[0]
    n = lax.axis_size("col")
    sizes = (members, levels, vectors, modes, columns)
    chunks = modes * vectors // LANES
    tiles = -(-chunks * members // n)
    rows = tiles * levels
    f32 = jnp.float32
    vmem = pl.BlockSpec(memory_space=pltpu.VMEM)

    terms, stat = pl.pallas_call(
        functools.partial(adjoint_kernel, sizes),
        out_shape=(
            jax.ShapeDtypeStruct((n * rows, LANES), f32),
            jax.ShapeDtypeStruct((8, LANES), f32),
        ),
        in_specs=[vmem] * 4,
        out_specs=(vmem, vmem),
        name="adjoint",
    )(perturbations, gradient, horizontal, area.reshape(1, columns))

    vert = vertical * (columns * n)
    vert_t = jnp.pad(vertical.T, ((0, 0), (0, LANES - vmodes)))
    vert = jnp.pad(vert, ((0, 0), (0, LANES - levels)))
    dma = pltpu.SemaphoreType.DMA
    lifted, parts, total = pl.pallas_call(
        functools.partial(exchange_kernel, sizes, n),
        out_shape=(
            jax.ShapeDtypeStruct((n, rows, LANES), f32),
            jax.ShapeDtypeStruct((n, 8, LANES), f32),
            jax.ShapeDtypeStruct((8, LANES), f32),
        ),
        in_specs=[vmem] * 4,
        out_specs=(vmem, vmem, vmem),
        scratch_shapes=[
            pltpu.VMEM((n, rows, LANES), f32),
            pltpu.VMEM((n, 8, LANES), f32),
            pltpu.VMEM((2, rows, LANES), f32),
            pltpu.VMEM((2, vmodes, LANES), f32),
            pltpu.VMEM((8, LANES), f32),
            dma((n,)), dma((n,)), dma((n,)), dma((n,)),
            dma((n,)), dma((n,)), dma((n,)), dma((n,)),
            dma((2,)), dma((2,)),
        ],
        compiler_params=pltpu.CompilerParams(collective_id=0, has_side_effects=True),
        name="exchange",
    )(terms.reshape(n, rows, LANES), stat, vert, vert_t)

    increment, background = pl.pallas_call(
        functools.partial(forward_kernel, sizes, n),
        out_shape=(
            jax.ShapeDtypeStruct((vectors, levels, columns), f32),
            jax.ShapeDtypeStruct((8, LANES), f32),
        ),
        in_specs=[vmem] * 5,
        out_specs=(vmem, vmem),
        scratch_shapes=[pltpu.VMEM((modes, columns), f32)],
        name="forward",
    )(lifted.reshape(n * rows, LANES), parts, total, perturbations, horizontal)
    return increment, background[0, :vectors]


def solution(mesh):
    return jax.shard_map(
        per_device,
        mesh=mesh,
        in_specs=(
            P(None, "lev", "col"),
            P(None, "lev", "col"),
            P(None, "col"),
            P("col"),
            P(None, "lev"),
        ),
        out_specs=(P(None, "lev", "col"), P()),
        check_vma=False,
    )
```

```python
import functools

import jax
import jax.numpy as jnp
from jax import lax
from jax.experimental import pallas as pl
from jax.experimental.pallas import tpu as pltpu
from jax.sharding import PartitionSpec as P

LANES = 128
NT = (((1,), (1,)), ((), ()))
TN = (((0,), (0,)), ((), ()))
NN = (((1,), (0,)), ((), ()))


def split(x):
    high = x.astype(jnp.bfloat16)
    low = (x - high.astype(jnp.float32)).astype(jnp.bfloat16)
    return high, low


def adjoint_kernel(sizes, pert_ref, grad_ref, hor_ref, area_ref, terms_ref, stat_ref):
    members, levels, vectors, modes, columns = sizes
    group = LANES // vectors
    chunks = modes // group
    used = chunks * members * levels
    if used < terms_ref.shape[0]:
        terms_ref[used:, :] = jnp.zeros((terms_ref.shape[0] - used, LANES), jnp.float32)
    area = area_ref[...]
    power = jnp.sum(area * hor_ref[...] * hor_ref[...], axis=1, keepdims=True)
    spread_power = jnp.broadcast_to(power, (modes, LANES))
    lane = lax.broadcasted_iota(jnp.int32, (modes, LANES), 1)
    row = lax.broadcasted_iota(jnp.int32, (modes, LANES), 0)
    powers = jnp.sum(jnp.where(lane == row, spread_power, 0.0), axis=0, keepdims=True)
    total = jnp.broadcast_to(jnp.sum(area, axis=1, keepdims=True), (1, LANES))
    stat_row = jnp.where(lane[:1] == modes, total, powers)
    stat_ref[...] = jnp.broadcast_to(stat_row, stat_ref.shape)

    def level(l, carry):
        high, low = split(pert_ref[:, l, :])
        both = jnp.concatenate([high, low], axis=0)
        weighted = grad_ref[:, l, :] * area
        for j in range(chunks):
            products = jnp.concatenate(
                [weighted * hor_ref[b : b + 1, :] for b in range(j * group, (j + 1) * group)],
                axis=0,
            )
            x = jnp.concatenate(split(products), axis=0)
            out = lax.dot_general(both, x, NT, preferred_element_type=jnp.float32)
            terms = out[:members, :LANES] + (out[members:, :LANES] + out[:members, LANES:])
            terms_ref[pl.ds(j * members * levels + l, members, stride=levels), :] = terms
        return carry

    for l in range(levels):
        level(l, 0)


def factor_column(stat, modes):
    lane = lax.broadcasted_iota(jnp.int32, (modes, LANES), 1)
    row = lax.broadcasted_iota(jnp.int32, (modes, LANES), 0)
    wide = jnp.broadcast_to(stat, (modes, LANES))
    power = jnp.sum(jnp.where(lane == row, wide, 0.0), axis=1, keepdims=True)
    area = jnp.sum(jnp.where(lane == modes, wide, 0.0), axis=1, keepdims=True)
    return 1.0 / jnp.sqrt(modes * (power / area + 1e-06)), area


def exchange_kernel(
    sizes, n, terms_ref, stat_ref, vert_ref, vert_t_ref, lifted_ref, parts_ref, total_ref,
    first_a, first_b, second, third, stats, reduced, verticals, weights,
    send_h, recv_h, send_g, recv_g, send_s, recv_s, send_l, recv_l, send_b, recv_b,
    send_p, recv_p,
):
    members, levels, vectors, modes, columns = sizes
    group = LANES // vectors
    chunks = modes // group
    vmodes = vert_ref.shape[0]
    rows = terms_ref.shape[3]
    tiles = rows // levels
    outer = n // 4
    rows_a = first_a.shape[2]
    half_a = pl.ds(0, rows_a)
    half_b = pl.ds(rows_a, rows - rows_a)
    me = lax.axis_index("col")
    lev = lax.axis_index("lev")
    other = 1 - lev
    x = lax.rem(me, 2)
    y = lax.rem(lax.div(me, 2), 2)
    h = lax.div(me, 4)
    not_x, not_y = 1 - x, 1 - y
    x_peer = (4 * h + 2 * y + not_x, lev)
    y_peer = (4 * h + 2 * not_y + x, lev)
    mesh_id = pl.DeviceIdType.MESH
    barrier = pltpu.get_barrier_semaphore()

    def greet(p, carry):
        pl.semaphore_signal(
            barrier, inc=1, device_id=(lax.rem(me + p, n), lev), device_id_type=mesh_id
        )
        return carry

    lax.fori_loop(1, n, greet, 0)
    pl.semaphore_signal(barrier, inc=1, device_id=(me, other), device_id_type=mesh_id)
    pl.semaphore_wait(barrier, n)

    def remote(src, dst, send, recv, device):
        return pltpu.make_async_remote_copy(
            src_ref=src, dst_ref=dst, send_sem=send, recv_sem=recv,
            device_id=device, device_id_type=mesh_id,
        )

    def half_copy(i, src, dst, device):
        return remote(src, dst, send_h.at[i], recv_h.at[i], device)

    def outer_copy(p):
        there = lax.rem(h + p, outer)
        device = (4 * there + 2 * y + x, lev)
        return remote(second.at[there], third.at[p], send_g.at[p], recv_g.at[p], device)

    def stat_copy(p, slot):
        peer = lax.rem(me + p, n)
        return remote(stat_ref, stats.at[slot], send_s.at[p], recv_s.at[p], (peer, lev))

    def lifted_copy(p, slot):
        there = lax.rem(h + p, outer)
        device = (4 * there + 2 * y + x, lev)
        block = lifted_ref.at[slot, y, x]
        return remote(block, block, send_l.at[p], recv_l.at[p], device)

    def part_copy(p, slot):
        peer = lax.rem(me + p, n)
        return remote(
            parts_ref.at[slot], parts_ref.at[slot], send_b.at[p], recv_b.at[p], (peer, lev)
        )

    one_a = half_copy(0, terms_ref.at[:, :, not_x, half_a], first_a, x_peer)
    one_b = half_copy(1, terms_ref.at[:, not_y, :, half_b], first_b, y_peer)
    one_a.start()
    one_b.start()

    def start_stats(p, carry):
        stat_copy(p, me).start()
        return carry

    lax.fori_loop(1, n, start_stats, 0)
    vert_copy = remote(
        vert_ref, verticals.at[lev], send_p.at[0], recv_p.at[0], (me, other)
    )
    vert_copy.start()
    stats[me] = stat_ref[...]
    verticals[lev] = vert_ref[...]

    def add_a(i, carry):
        first_a[i, not_y] += terms_ref[i, not_y, x, half_a]
        return carry

    def add_b(i, carry):
        first_b[i, not_x] += terms_ref[i, y, not_x, half_b]
        return carry

    two_a = half_copy(2, first_a.at[:, not_y], second.at[:, half_a], y_peer)
    two_b = half_copy(3, first_b.at[:, not_x], second.at[:, half_b], x_peer)
    one_a.wait_recv()
    lax.fori_loop(0, outer, add_a, 0)
    two_a.start()
    one_b.wait_recv()
    lax.fori_loop(0, outer, add_b, 0)
    two_b.start()

    def take_stats(p, carry):
        stat_copy(p, lax.rem(me + n - p, n)).wait_recv()
        return carry

    lax.fori_loop(1, n, take_stats, 0)
    two_a.wait_recv()
    two_b.wait_recv()

    def add_second(there):
        second[there, half_a] += terms_ref[there, y, x, half_a] + first_a[there, y]
        second[there, half_b] += terms_ref[there, y, x, half_b] + first_b[there, x]

    def send_outer(p, carry):
        add_second(lax.rem(h + p, outer))
        outer_copy(p).start()
        return carry

    lax.fori_loop(1, outer, send_outer, 0)
    add_second(h)
    reduced[lev] = second[h]

    def take(p, carry):
        outer_copy(p).wait_recv()
        reduced[lev] += third[p]
        return carry

    lax.fori_loop(1, outer, take, 0)
    pair_copy = remote(
        reduced.at[lev], reduced.at[lev], send_p.at[1], recv_p.at[1], (me, other)
    )
    pair_copy.start()

    def add_stat(i, carry):
        return carry + stats[i]

    stat = lax.fori_loop(0, n, add_stat, jnp.zeros(stat_ref.shape, jnp.float32))
    total_ref[...] = stat
    factor, area = factor_column(stat[:1], modes)
    factor = factor / area
    lane = lax.broadcasted_iota(jnp.int32, (modes, LANES), 1)
    row = lax.broadcasted_iota(jnp.int32, (modes, LANES), 0)
    placed = jnp.where(
        lax.div(lane, vectors) == lax.rem(row, group), jnp.broadcast_to(factor, lane.shape), 0.0
    )
    for j in range(chunks):
        weights[j : j + 1, :] = jnp.sum(
            placed[j * group : (j + 1) * group], axis=0, keepdims=True
        )
    remote(
        vert_ref, verticals.at[other], send_p.at[0], recv_p.at[0], (me, other)
    ).wait_recv()
    remote(
        reduced.at[lev], reduced.at[other], send_p.at[1], recv_p.at[1], (me, other)
    ).wait_recv()

    def wide(index):
        block = reduced[index]
        return jnp.concatenate(
            [block[i * levels : (i + 1) * levels] for i in range(tiles)], axis=1
        )

    def dot(a, b):
        return lax.dot_general(
            a, b, NN, precision=lax.Precision.HIGHEST, preferred_element_type=jnp.float32
        )

    control = dot(verticals[0][:, :levels], wide(0)) + dot(verticals[1][:, :levels], wide(1))
    lifted = dot(vert_t_ref[...][:, :vmodes], control)
    part = jnp.zeros((1, LANES), jnp.float32)
    for i in range(tiles):
        lifted_ref[h, y, x, i * levels : (i + 1) * levels, :] = lifted[:, i * LANES : (i + 1) * LANES]
        chunk = jnp.minimum(lax.div(me * tiles + i, members), chunks - 1)
        scaled = control[:, i * LANES : (i + 1) * LANES] * weights[pl.ds(chunk, 1), :]
        part = part + jnp.sum(scaled * scaled, axis=0, keepdims=True)
    parts_ref[me] = jnp.broadcast_to(part, parts_ref.shape[1:])

    def start_lifted(p, carry):
        lifted_copy(p, h).start()
        return carry

    def start_parts(p, carry):
        part_copy(p, me).start()
        return carry

    def take_lifted(p, carry):
        lifted_copy(p, lax.rem(h + outer - p, outer)).wait_recv()
        return carry

    lax.fori_loop(1, outer, start_lifted, 0)
    lax.fori_loop(1, n, start_parts, 0)
    lax.fori_loop(1, outer, take_lifted, 0)

    def gather_copy(i, block, device):
        return half_copy(i, block, block, device)

    three_a = gather_copy(4, lifted_ref.at[:, y, x, half_a], y_peer)
    three_b = gather_copy(5, lifted_ref.at[:, y, x, half_b], x_peer)
    three_a.start()
    three_b.start()
    four_a = gather_copy(6, lifted_ref.at[:, :, x, half_a], x_peer)
    four_b = gather_copy(7, lifted_ref.at[:, y, :, half_b], y_peer)
    gather_copy(4, lifted_ref.at[:, not_y, x, half_a], y_peer).wait_recv()
    four_a.start()
    gather_copy(5, lifted_ref.at[:, y, not_x, half_b], x_peer).wait_recv()
    four_b.start()
    for copy in (one_a, one_b, two_a, two_b, three_a, three_b, vert_copy, pair_copy):
        copy.wait_send()

    def finish(p, carry):
        stat_copy(p, me).wait_send()
        part_copy(p, lax.rem(me + n - p, n)).wait_recv()
        part_copy(p, me).wait_send()
        return carry

    def finish_outer(p, carry):
        outer_copy(p).wait_send()
        lifted_copy(p, h).wait_send()
        return carry

    lax.fori_loop(1, n, finish, 0)
    lax.fori_loop(1, outer, finish_outer, 0)
    gather_copy(6, lifted_ref.at[:, :, not_x, half_a], x_peer).wait_recv()
    gather_copy(7, lifted_ref.at[:, not_y, :, half_b], y_peer).wait_recv()
    four_a.wait_send()
    four_b.wait_send()


def forward_kernel(
    sizes, n, lifted_ref, parts_ref, total_ref, pert_ref, hor_ref, out_ref, bg_ref, scaled_ref
):
    members, levels, vectors, modes, columns = sizes
    group = LANES // vectors
    chunks = modes // group
    width = 256
    part = lax.fori_loop(
        0, n, lambda i, c: c + parts_ref[i], jnp.zeros(parts_ref.shape[1:], jnp.float32)
    )
    folded = part
    for g in range(1, group):
        folded = folded + pltpu.roll(part, g * vectors, 1)
    bg_ref[...] = 0.5 * folded
    factor, area = factor_column(total_ref[:1, :], modes)
    scaled_ref[...] = hor_ref[...] * (factor * (factor / area))

    def level(l, carry):
        lhs = []
        for j in range(chunks):
            high, low = split(
                lifted_ref[pl.ds(j * members * levels + l, members, stride=levels), :]
            )
            lhs.append(jnp.concatenate([high, low, high], axis=0))
        for c in range(0, columns, width):
            high, low = split(pert_ref[:, l, c : c + width])
            rhs = jnp.concatenate([high, high, low], axis=0)
            acc = None
            for j in range(chunks):
                spread = lax.dot_general(lhs[j], rhs, TN, preferred_element_type=jnp.float32)
                for g in range(group):
                    b = j * group + g
                    term = (
                        spread[g * vectors : (g + 1) * vectors]
                        * scaled_ref[b : b + 1, c : c + width]
                    )
                    acc = term if acc is None else acc + term
            out_ref[:, l, c : c + width] = acc
        return carry

    for l in range(levels):
        level(l, 0)


def per_device(perturbations, gradient, horizontal, area, vertical):
    members, levels, columns = perturbations.shape
    vectors = gradient.shape[0]
    modes = horizontal.shape[0]
    vmodes = vertical.shape[0]
    n = lax.axis_size("col")
    sizes = (members, levels, vectors, modes, columns)
    chunks = modes * vectors // LANES
    tiles = -(-chunks * members // n)
    rows = tiles * levels
    outer = n // 4
    rows_a = (tiles + 1) // 2 * levels
    f32 = jnp.float32
    vmem = pl.BlockSpec(memory_space=pltpu.VMEM)

    terms, stat = pl.pallas_call(
        functools.partial(adjoint_kernel, sizes),
        out_shape=(
            jax.ShapeDtypeStruct((n * rows, LANES), f32),
            jax.ShapeDtypeStruct((8, LANES), f32),
        ),
        in_specs=[vmem] * 4,
        out_specs=(vmem, vmem),
        name="adjoint",
    )(perturbations, gradient, horizontal, area.reshape(1, columns))

    vert = vertical * (columns * n)
    vert_t = jnp.pad(vertical.T, ((0, 0), (0, LANES - vmodes)))
    vert = jnp.pad(vert, ((0, 0), (0, LANES - levels)))
    dma = pltpu.SemaphoreType.DMA
    lifted, parts, total = pl.pallas_call(
        functools.partial(exchange_kernel, sizes, n),
        out_shape=(
            jax.ShapeDtypeStruct((outer, 2, 2, rows, LANES), f32),
            jax.ShapeDtypeStruct((n, 8, LANES), f32),
            jax.ShapeDtypeStruct((8, LANES), f32),
        ),
        in_specs=[vmem] * 4,
        out_specs=(vmem, vmem, vmem),
        scratch_shapes=[
            pltpu.VMEM((outer, 2, rows_a, LANES), f32),
            pltpu.VMEM((outer, 2, rows - rows_a, LANES), f32),
            pltpu.VMEM((outer, rows, LANES), f32),
            pltpu.VMEM((outer, rows, LANES), f32),
            pltpu.VMEM((n, 8, LANES), f32),
            pltpu.VMEM((2, rows, LANES), f32),
            pltpu.VMEM((2, vmodes, LANES), f32),
            pltpu.VMEM((8, LANES), f32),
            dma((8,)), dma((8,)), dma((outer,)), dma((outer,)), dma((n,)), dma((n,)),
            dma((outer,)), dma((outer,)), dma((n,)), dma((n,)),
            dma((2,)), dma((2,)),
        ],
        compiler_params=pltpu.CompilerParams(collective_id=0, has_side_effects=True),
        name="exchange",
    )(terms.reshape(outer, 2, 2, rows, LANES), stat, vert, vert_t)

    increment, background = pl.pallas_call(
        functools.partial(forward_kernel, sizes, n),
        out_shape=(
            jax.ShapeDtypeStruct((vectors, levels, columns), f32),
            jax.ShapeDtypeStruct((8, LANES), f32),
        ),
        in_specs=[vmem] * 5,
        out_specs=(vmem, vmem),
        scratch_shapes=[pltpu.VMEM((modes, columns), f32)],
        name="forward",
    )(lifted.reshape(n * rows, LANES), parts, total, perturbations, horizontal)
    return increment, background[0, :vectors]


def solution(mesh):
    return jax.shard_map(
        per_device,
        mesh=mesh,
        in_specs=(
            P(None, "lev", "col"),
            P(None, "lev", "col"),
            P(None, "col"),
            P("col"),
            P(None, "lev"),
        ),
        out_specs=(P(None, "lev", "col"), P()),
        check_vma=False,
    )
```

```python
import functools

import jax
import jax.numpy as jnp
from jax import lax
from jax.experimental import pallas as pl
from jax.experimental.pallas import tpu as pltpu
from jax.sharding import PartitionSpec as P

LANES = 128
NT = (((1,), (1,)), ((), ()))
TN = (((0,), (0,)), ((), ()))
NN = (((1,), (0,)), ((), ()))


def split(x):
    high = x.astype(jnp.bfloat16)
    low = (x - high.astype(jnp.float32)).astype(jnp.bfloat16)
    return high, low


def adjoint_kernel(sizes, pert_ref, grad_ref, hor_ref, area_ref, terms_ref, stat_ref):
    members, levels, vectors, modes, columns = sizes
    group = LANES // vectors
    chunks = modes // group
    used = chunks * members * levels
    if used < terms_ref.shape[0]:
        terms_ref[used:, :] = jnp.zeros((terms_ref.shape[0] - used, LANES), jnp.float32)
    area = area_ref[...]
    power = jnp.sum(area * hor_ref[...] * hor_ref[...], axis=1, keepdims=True)
    spread_power = jnp.broadcast_to(power, (modes, LANES))
    lane = lax.broadcasted_iota(jnp.int32, (modes, LANES), 1)
    row = lax.broadcasted_iota(jnp.int32, (modes, LANES), 0)
    powers = jnp.sum(jnp.where(lane == row, spread_power, 0.0), axis=0, keepdims=True)
    total = jnp.broadcast_to(jnp.sum(area, axis=1, keepdims=True), (1, LANES))
    stat_row = jnp.where(lane[:1] == modes, total, powers)
    stat_ref[...] = jnp.broadcast_to(stat_row, stat_ref.shape)

    def level(l, carry):
        high, low = split(pert_ref[:, l, :])
        both = jnp.concatenate([high, low], axis=0)
        weighted = grad_ref[:, l, :] * area
        for j in range(chunks):
            products = jnp.concatenate(
                [weighted * hor_ref[b : b + 1, :] for b in range(j * group, (j + 1) * group)],
                axis=0,
            )
            x = jnp.concatenate(split(products), axis=0)
            out = lax.dot_general(both, x, NT, preferred_element_type=jnp.float32)
            terms = out[:members, :LANES] + (out[members:, :LANES] + out[:members, LANES:])
            terms_ref[pl.ds(j * members * levels + l, members, stride=levels), :] = terms
        return carry

    for l in range(levels):
        level(l, 0)


def factor_column(stat, modes):
    lane = lax.broadcasted_iota(jnp.int32, (modes, LANES), 1)
    row = lax.broadcasted_iota(jnp.int32, (modes, LANES), 0)
    wide = jnp.broadcast_to(stat, (modes, LANES))
    power = jnp.sum(jnp.where(lane == row, wide, 0.0), axis=1, keepdims=True)
    area = jnp.sum(jnp.where(lane == modes, wide, 0.0), axis=1, keepdims=True)
    return 1.0 / jnp.sqrt(modes * (power / area + 1e-06)), area


def exchange_kernel(
    sizes, n, terms_ref, stat_ref, vert_ref, vert_t_ref, lifted_ref, parts_ref, total_ref,
    first_a, first_b, second, third, stats, reduced, verticals, weights,
    send_h, recv_h, send_g, recv_g, send_s, recv_s, send_l, recv_l, send_b, recv_b,
    send_p, recv_p,
):
    members, levels, vectors, modes, columns = sizes
    group = LANES // vectors
    chunks = modes // group
    vmodes = vert_ref.shape[0]
    rows = terms_ref.shape[3]
    tiles = rows // levels
    outer = n // 4
    rows_a = first_a.shape[2]
    half_a = pl.ds(0, rows_a)
    half_b = pl.ds(rows_a, rows - rows_a)
    me = lax.axis_index("col")
    lev = lax.axis_index("lev")
    other = 1 - lev
    x = lax.rem(me, 2)
    y = lax.rem(lax.div(me, 2), 2)
    h = lax.div(me, 4)
    not_x, not_y = 1 - x, 1 - y
    x_peer = (4 * h + 2 * y + not_x, lev)
    y_peer = (4 * h + 2 * not_y + x, lev)
    mesh_id = pl.DeviceIdType.MESH
    barrier = pltpu.get_barrier_semaphore()

    def greet(p, carry):
        pl.semaphore_signal(
            barrier, inc=1, device_id=(lax.rem(me + p, n), lev), device_id_type=mesh_id
        )
        return carry

    lax.fori_loop(1, n, greet, 0)
    pl.semaphore_signal(barrier, inc=1, device_id=(me, other), device_id_type=mesh_id)
    pl.semaphore_wait(barrier, n)

    def remote(src, dst, send, recv, device):
        return pltpu.make_async_remote_copy(
            src_ref=src, dst_ref=dst, send_sem=send, recv_sem=recv,
            device_id=device, device_id_type=mesh_id,
        )

    def half_copy(i, src, dst, device):
        return remote(src, dst, send_h.at[i], recv_h.at[i], device)

    def outer_copy(p):
        there = lax.rem(h + p, outer)
        device = (4 * there + 2 * y + x, lev)
        return remote(second.at[there], third.at[p], send_g.at[p], recv_g.at[p], device)

    def stat_copy(p, slot):
        peer = lax.rem(me + p, n)
        return remote(stat_ref, stats.at[slot], send_s.at[p], recv_s.at[p], (peer, lev))

    def lifted_copy(p, slot):
        there = lax.rem(h + p, outer)
        device = (4 * there + 2 * y + x, lev)
        block = lifted_ref.at[slot, y, x]
        return remote(block, block, send_l.at[p], recv_l.at[p], device)

    def part_copy(p, slot):
        peer = lax.rem(me + p, n)
        return remote(
            parts_ref.at[slot], parts_ref.at[slot], send_b.at[p], recv_b.at[p], (peer, lev)
        )

    one_a = half_copy(0, terms_ref.at[:, :, not_x, half_a], first_a, x_peer)
    one_b = half_copy(1, terms_ref.at[:, not_y, :, half_b], first_b, y_peer)
    one_a.start()
    one_b.start()

    def start_stats(p, carry):
        stat_copy(p, me).start()
        return carry

    lax.fori_loop(1, n, start_stats, 0)
    vert_copy = remote(
        vert_ref, verticals.at[lev], send_p.at[0], recv_p.at[0], (me, other)
    )
    vert_copy.start()
    stats[me] = stat_ref[...]
    verticals[lev] = vert_ref[...]

    def add_a(i, carry):
        first_a[i, not_y] += terms_ref[i, not_y, x, half_a]
        return carry

    def add_b(i, carry):
        first_b[i, not_x] += terms_ref[i, y, not_x, half_b]
        return carry

    two_a = half_copy(2, first_a.at[:, not_y], second.at[:, half_a], y_peer)
    two_b = half_copy(3, first_b.at[:, not_x], second.at[:, half_b], x_peer)
    one_a.wait_recv()
    lax.fori_loop(0, outer, add_a, 0)
    two_a.start()
    one_b.wait_recv()
    lax.fori_loop(0, outer, add_b, 0)
    two_b.start()

    def take_stats(p, carry):
        stat_copy(p, lax.rem(me + n - p, n)).wait_recv()
        return carry

    lax.fori_loop(1, n, take_stats, 0)
    two_a.wait_recv()
    two_b.wait_recv()

    def add_second(there):
        second[there, half_a] += terms_ref[there, y, x, half_a] + first_a[there, y]
        second[there, half_b] += terms_ref[there, y, x, half_b] + first_b[there, x]

    def send_outer(p, carry):
        add_second(lax.rem(h + p, outer))
        outer_copy(p).start()
        return carry

    lax.fori_loop(1, outer, send_outer, 0)
    add_second(h)
    reduced[lev] = second[h]

    def take(p, carry):
        outer_copy(p).wait_recv()
        reduced[lev] += third[p]
        return carry

    lax.fori_loop(1, outer, take, 0)
    pair_copy = remote(
        reduced.at[lev], reduced.at[lev], send_p.at[1], recv_p.at[1], (me, other)
    )
    pair_copy.start()

    def add_stat(i, carry):
        return carry + stats[i]

    stat = lax.fori_loop(0, n, add_stat, jnp.zeros(stat_ref.shape, jnp.float32))
    total_ref[...] = stat
    factor, area = factor_column(stat[:1], modes)
    factor = factor / area
    lane = lax.broadcasted_iota(jnp.int32, (modes, LANES), 1)
    row = lax.broadcasted_iota(jnp.int32, (modes, LANES), 0)
    placed = jnp.where(
        lax.div(lane, vectors) == lax.rem(row, group), jnp.broadcast_to(factor, lane.shape), 0.0
    )
    for j in range(chunks):
        weights[j : j + 1, :] = jnp.sum(
            placed[j * group : (j + 1) * group], axis=0, keepdims=True
        )
    remote(
        vert_ref, verticals.at[other], send_p.at[0], recv_p.at[0], (me, other)
    ).wait_recv()
    remote(
        reduced.at[lev], reduced.at[other], send_p.at[1], recv_p.at[1], (me, other)
    ).wait_recv()

    def wide(index):
        block = reduced[index]
        return jnp.concatenate(
            [block[i * levels : (i + 1) * levels] for i in range(tiles)], axis=1
        )

    def dot(a, b):
        return lax.dot_general(
            a, b, NN, precision=lax.Precision.HIGHEST, preferred_element_type=jnp.float32
        )

    control = dot(verticals[0][:, :levels], wide(0)) + dot(verticals[1][:, :levels], wide(1))
    lifted = lax.dot_general(
        vert_t_ref[...], control, TN, precision=lax.Precision.HIGHEST,
        preferred_element_type=jnp.float32,
    )
    part = jnp.zeros((1, LANES), jnp.float32)
    for i in range(tiles):
        lifted_ref[h, y, x, i * levels : (i + 1) * levels, :] = lifted[:, i * LANES : (i + 1) * LANES]
        chunk = jnp.minimum(lax.div(me * tiles + i, members), chunks - 1)
        scaled = control[:, i * LANES : (i + 1) * LANES] * weights[pl.ds(chunk, 1), :]
        part = part + jnp.sum(scaled * scaled, axis=0, keepdims=True)
    parts_ref[me] = jnp.broadcast_to(part, parts_ref.shape[1:])

    def start_lifted(p, carry):
        lifted_copy(p, h).start()
        return carry

    def start_parts(p, carry):
        part_copy(p, me).start()
        return carry

    def take_lifted(p, carry):
        lifted_copy(p, lax.rem(h + outer - p, outer)).wait_recv()
        return carry

    lax.fori_loop(1, outer, start_lifted, 0)
    lax.fori_loop(1, n, start_parts, 0)
    lax.fori_loop(1, outer, take_lifted, 0)

    def gather_copy(i, block, device):
        return half_copy(i, block, block, device)

    three_a = gather_copy(4, lifted_ref.at[:, y, x, half_a], y_peer)
    three_b = gather_copy(5, lifted_ref.at[:, y, x, half_b], x_peer)
    three_a.start()
    three_b.start()
    four_a = gather_copy(6, lifted_ref.at[:, :, x, half_a], x_peer)
    four_b = gather_copy(7, lifted_ref.at[:, y, :, half_b], y_peer)
    gather_copy(4, lifted_ref.at[:, not_y, x, half_a], y_peer).wait_recv()
    four_a.start()
    gather_copy(5, lifted_ref.at[:, y, not_x, half_b], x_peer).wait_recv()
    four_b.start()
    for copy in (one_a, one_b, two_a, two_b, three_a, three_b, vert_copy, pair_copy):
        copy.wait_send()

    def finish(p, carry):
        stat_copy(p, me).wait_send()
        part_copy(p, lax.rem(me + n - p, n)).wait_recv()
        part_copy(p, me).wait_send()
        return carry

    def finish_outer(p, carry):
        outer_copy(p).wait_send()
        lifted_copy(p, h).wait_send()
        return carry

    lax.fori_loop(1, n, finish, 0)
    lax.fori_loop(1, outer, finish_outer, 0)
    gather_copy(6, lifted_ref.at[:, :, not_x, half_a], x_peer).wait_recv()
    gather_copy(7, lifted_ref.at[:, not_y, :, half_b], y_peer).wait_recv()
    four_a.wait_send()
    four_b.wait_send()


def forward_kernel(
    sizes, n, lifted_ref, parts_ref, total_ref, pert_ref, hor_ref, out_ref, bg_ref, scaled_ref
):
    members, levels, vectors, modes, columns = sizes
    group = LANES // vectors
    chunks = modes // group
    width = 256
    part = lax.fori_loop(
        0, n, lambda i, c: c + parts_ref[i], jnp.zeros(parts_ref.shape[1:], jnp.float32)
    )
    folded = part
    for g in range(1, group):
        folded = folded + pltpu.roll(part, g * vectors, 1)
    bg_ref[...] = 0.5 * folded
    factor, area = factor_column(total_ref[:1, :], modes)
    scaled_ref[...] = hor_ref[...] * (factor * (factor / area))

    def level(l, carry):
        lhs = []
        for j in range(chunks):
            high, low = split(
                lifted_ref[pl.ds(j * members * levels + l, members, stride=levels), :]
            )
            lhs.append(jnp.concatenate([high, low, high], axis=0))
        for c in range(0, columns, width):
            high, low = split(pert_ref[:, l, c : c + width])
            rhs = jnp.concatenate([high, high, low], axis=0)
            acc = None
            for j in range(chunks):
                spread = lax.dot_general(lhs[j], rhs, TN, preferred_element_type=jnp.float32)
                for g in range(group):
                    b = j * group + g
                    term = (
                        spread[g * vectors : (g + 1) * vectors]
                        * scaled_ref[b : b + 1, c : c + width]
                    )
                    acc = term if acc is None else acc + term
            out_ref[:, l, c : c + width] = acc
        return carry

    for l in range(levels):
        level(l, 0)


def per_device(perturbations, gradient, horizontal, area, vertical):
    members, levels, columns = perturbations.shape
    vectors = gradient.shape[0]
    modes = horizontal.shape[0]
    vmodes = vertical.shape[0]
    n = lax.axis_size("col")
    sizes = (members, levels, vectors, modes, columns)
    chunks = modes * vectors // LANES
    tiles = -(-chunks * members // n)
    rows = tiles * levels
    outer = n // 4
    rows_a = (tiles + 1) // 2 * levels
    f32 = jnp.float32
    vmem = pl.BlockSpec(memory_space=pltpu.VMEM)

    terms, stat = pl.pallas_call(
        functools.partial(adjoint_kernel, sizes),
        out_shape=(
            jax.ShapeDtypeStruct((n * rows, LANES), f32),
            jax.ShapeDtypeStruct((8, LANES), f32),
        ),
        in_specs=[vmem] * 4,
        out_specs=(vmem, vmem),
        name="adjoint",
    )(perturbations, gradient, horizontal, area.reshape(1, columns))

    vert = vertical * (columns * n)
    vert = jnp.pad(vert, ((0, 0), (0, LANES - levels)))
    dma = pltpu.SemaphoreType.DMA
    lifted, parts, total = pl.pallas_call(
        functools.partial(exchange_kernel, sizes, n),
        out_shape=(
            jax.ShapeDtypeStruct((outer, 2, 2, rows, LANES), f32),
            jax.ShapeDtypeStruct((n, 8, LANES), f32),
            jax.ShapeDtypeStruct((8, LANES), f32),
        ),
        in_specs=[vmem] * 4,
        out_specs=(vmem, vmem, vmem),
        scratch_shapes=[
            pltpu.VMEM((outer, 2, rows_a, LANES), f32),
            pltpu.VMEM((outer, 2, rows - rows_a, LANES), f32),
            pltpu.VMEM((outer, rows, LANES), f32),
            pltpu.VMEM((outer, rows, LANES), f32),
            pltpu.VMEM((n, 8, LANES), f32),
            pltpu.VMEM((2, rows, LANES), f32),
            pltpu.VMEM((2, vmodes, LANES), f32),
            pltpu.VMEM((8, LANES), f32),
            dma((8,)), dma((8,)), dma((outer,)), dma((outer,)), dma((n,)), dma((n,)),
            dma((outer,)), dma((outer,)), dma((n,)), dma((n,)),
            dma((2,)), dma((2,)),
        ],
        compiler_params=pltpu.CompilerParams(collective_id=0, has_side_effects=True),
        name="exchange",
    )(terms.reshape(outer, 2, 2, rows, LANES), stat, vert, vertical)

    increment, background = pl.pallas_call(
        functools.partial(forward_kernel, sizes, n),
        out_shape=(
            jax.ShapeDtypeStruct((vectors, levels, columns), f32),
            jax.ShapeDtypeStruct((8, LANES), f32),
        ),
        in_specs=[vmem] * 5,
        out_specs=(vmem, vmem),
        scratch_shapes=[pltpu.VMEM((modes, columns), f32)],
        name="forward",
    )(lifted.reshape(n * rows, LANES), parts, total, perturbations, horizontal)
    return increment, background[0, :vectors]


def solution(mesh):
    return jax.shard_map(
        per_device,
        mesh=mesh,
        in_specs=(
            P(None, "lev", "col"),
            P(None, "lev", "col"),
            P(None, "col"),
            P("col"),
            P(None, "lev"),
        ),
        out_specs=(P(None, "lev", "col"), P()),
        check_vma=False,
    )
```
